256 devices in a mesh: clusters: 8 (over y, x_hi), members: 32 (over z, x_lo, core).
Axes of the slice: x: 4 (x_hi: 2, x_lo: 2; x = x_hi * 2 + x_lo), y: 4, z: 8, core: 2. Of those that a mesh axis runs over, the one named last changes fastest.
Arguments:
- embeddings: float32 [131072, 1024], P(('clusters', 'members')), parts along dimension 0, as said below
- member_order: int32 [131072], P(('clusters', 'members')), parts along dimension 0, may hold values from 0 to 16383, each once
- threshold: float32 [8], P('clusters'), parts along dimension 0, may hold values from 0.25 to 0.5
Outputs:
- best_similarity: float32 [131072], P(('clusters', 'members')), parts along dimension 0
- excess: float32 [131072], P(('clusters', 'members')), parts along dimension 0
The draws below stay inside these ranges and needn't reach their ends.
There are 8 independent parts, one for each index of `clusters`. The reference program is written for one: setup_inputs(seed, part) draws one part's arguments, and reference() takes and returns one part's arrays. A program takes and returns all parts, laid end to end along the dimension named above; each array names one. Nothing has to cross between parts.
Inputs may be any that keep to these rules, and one draw needn't show every extreme that they name: member_order holds each of 0 to 16383 once. real-valued embeddings.
All inputs are finite; a program needn't handle non-finite values.
Results may differ from the reference program's by a relative error of at most 0.00051.
Values may be sent and summed in bfloat16 or wider, within the bound.
A program may use at most 128 MiB of HBM per device.

```python
import math
import jax
import jax.numpy as jnp
from jax import lax

E = 1024
MEMBERS = 16384


def draw_embeddings(key, part):
    keys = jax.random.split(key, 4)
    groups = MEMBERS // 4
    protos = jax.random.normal(keys[0], (groups, E), jnp.float32)
    group_id = jax.random.randint(keys[1], (MEMBERS,), 0, groups)
    mixing = jax.random.uniform(keys[2], (MEMBERS, 1), jnp.float32, 0.0, 2.5)
    noise = jax.random.normal(keys[3], (MEMBERS, E), jnp.float32)
    values = protos[group_id] * mixing + noise
    return values.astype(jnp.float32)


def setup_inputs(seed: int = 0, part: int = 0) -> dict:
    key_list = jax.random.split(jax.random.key(seed), 4)
    part_keys = jax.random.split(jax.random.fold_in(key_list[3], part), 4)
    return {
        "embeddings": draw_embeddings(jax.random.fold_in(jax.random.fold_in(key_list[3], part), 71), part),
        "member_order": jax.random.permutation(part_keys[1], MEMBERS).astype(jnp.int32),
        "threshold": jnp.clip(jax.random.uniform(part_keys[2], (1,), jnp.float32, 0.25, 0.5), 0.25, 0.5),
    }


def reference(embeddings, member_order, threshold):
    unit = (embeddings * lax.rsqrt(lax.optimization_barrier(jnp.sum(embeddings * embeddings, axis=1, keepdims=True)) + 1e-06)).astype(jnp.bfloat16)
    total = unit.shape[0]
    block = math.gcd(total, 512)
    rows = unit.reshape(total // block, block, unit.shape[1])
    orders = member_order.reshape(total // block, block)

    def one_block(pair):
        part_rows, part_order = pair
        sim = jnp.dot(part_rows, unit.T, preferred_element_type=jnp.float32)
        mask = member_order[None, :] < part_order[:, None]
        picked = jnp.where(mask, sim, jnp.float32(-1.0))
        return jnp.maximum(lax.optimization_barrier(jnp.max(picked, axis=1)), jnp.float32(-1.0))
    best = lax.map(one_block, (rows, orders)).reshape(total)
    excess = jnp.maximum(best - threshold[0], jnp.float32(0.0))
    return (best, excess)
```

```python
import functools

import jax
import jax.numpy as jnp
from jax import lax
from jax.experimental import pallas as pl
from jax.experimental.pallas import tpu as pltpu
from jax.sharding import PartitionSpec as P

MESH = pl.DeviceIdType.MESH
F32 = jnp.float32
BF16 = jnp.bfloat16

SO, SP1, SM1, SM2, SP2 = range(5)
BO, BX1, BP2, BXH, NB = 0, 4, 8, 12, 14
DM1, DP1, DOO, DM2, DP2, DX1, DXH, DP2O, DX1O, DXHO, ND = range(11)
VO, VP1, VM1, VM2, VP2, VX1, VXH, NV = 0, 2, 3, 4, 5, 7, 9, 11
RP1, RM1, RM2, RP2, RX1, RXHM, RXHP, NR = 0, 1, 2, 3, 5, 7, 9, 11
NC = 4


def kernel(
    order_ref, thr_ref, emb_ref, out_ref,
    stage, abuf, bbuf, racc, cacc, oa, ob, ordv, res, resin, fin,
    load_sem, send_sem, recv_sem, osend_sem, orecv_sem, rsend_sem, rrecv_sem,
):
    n = lax.axis_size("members")
    nz = n // 4
    me = lax.axis_index("members")
    z, x, c = me // 4, lax.rem(me // 2, 2), lax.rem(me, 2)
    xo, co = 1 - x, 1 - c
    ch = abuf.shape[1] // NC

    def dev(dz, px, pc):
        return {"members": lax.rem(z + dz + nz, nz) * 4 + px * 2 + pc}

    zq = lax.rem(z + 2, nz)
    upper = zq < nz // 2
    low = z < nz // 2

    loads = [
        pltpu.make_async_copy(emb_ref.at[pl.ds(j * ch, ch)], stage.at[j], load_sem.at[j]) for j in range(NC)
    ]
    for j in (0, 2, 1, 3):
        loads[j].start()

    peers = [dev(1, x, c), dev(-1, x, c), dev(0, x, co), dev(0, xo, c)]
    for h in (0, 1):
        peers += [dev(2, x, h), dev(-2, x, h), dev(2, xo, h), dev(-2, xo, h), dev(1, xo, h), dev(-1, xo, h)]
    barrier = pltpu.get_barrier_semaphore()
    for p in peers:
        pl.semaphore_signal(barrier, inc=1, device_id=p, device_id_type=MESH)

    def remote(kind, j, src, dst, target):
        return pltpu.make_async_remote_copy(
            src_ref=src, dst_ref=dst, send_sem=send_sem.at[kind, j], recv_sem=recv_sem.at[kind, j],
            device_id=target, device_id_type=MESH,
        )

    def rows(slot, j):
        return abuf.at[slot, pl.ds(pl.multiple_of(j * ch, ch), ch)]

    def half(tile, h):
        return bbuf.at[tile, pl.ds(pl.multiple_of(h * ch, ch), ch)]

    def c_m1(j):
        return remote(DM1, j, rows(SO, j), rows(SM1, j), dev(1, x, c))

    def c_p1(j):
        return remote(DP1, j, rows(SO, j), rows(SP1, j), dev(-1, x, c))

    def c_oo(j, h):
        return remote(DOO, j, rows(SO, j), half(BO + j, h), dev(0, x, co))

    def c_m2(j):
        return remote(DM2, j, rows(SM1, j), rows(SM2, j), dev(1, x, c))

    def c_p2(j):
        return remote(DP2, j, rows(SP1, j), half(BP2 + j, c), dev(-1, x, c))

    def c_x1(j):
        return remote(DX1, j, rows(SP1, j), half(BX1 + j, c), dev(0, xo, c))

    def c_xh_m(i):
        return remote(DXH, i, rows(SM2, i), half(BXH + i, c), dev(0, xo, c))

    def c_xh_p(i):
        return remote(DXH, i, half(BP2 + 2 + i, c), half(BXH + i, c), dev(0, xo, c))

    def c_fwd(kind, tile, j, h):
        return remote(kind, j, half(tile + j, h), half(tile + j, h), dev(0, x, co))

    def normalise(j):
        loads[j].wait()
        e = stage[j]
        u = (e * lax.rsqrt(jnp.sum(e * e, axis=1, keepdims=True) + 1e-06)).astype(BF16)
        abuf[SO, pl.ds(j * ch, ch)] = u
        bbuf[BO + j, pl.ds(pl.multiple_of(c * ch, ch), ch)] = u

    normalise(0)
    ordv[c] = order_ref[...]
    normalise(2)
    pl.semaphore_wait(barrier, len(peers))

    def order_copy(k, slot, target):
        return pltpu.make_async_remote_copy(
            src_ref=order_ref, dst_ref=ordv.at[slot], send_sem=osend_sem.at[k], recv_sem=orecv_sem.at[slot],
            device_id=target, device_id_type=MESH,
        )

    order_sends = [
        order_copy(0, VO + c, dev(0, x, co)), order_copy(1, VP1, dev(-1, x, c)), order_copy(2, VM1, dev(1, x, c)),
        order_copy(3, VM2, dev(2, x, c)),
    ]
    for h in (0, 1):
        order_sends += [order_copy(4 + h, VP2 + c, dev(-2, x, h)), order_copy(6 + h, VX1 + c, dev(-1, xo, h))]
    order_sends_low = []
    for h in (0, 1):
        order_sends_low += [order_copy(8 + h, VXH + c, dev(2, xo, h)), order_copy(10 + h, VXH + c, dev(-2, xo, h))]
    for o in order_sends:
        o.start()

    @pl.when(low)
    def _():
        for o in order_sends_low:
            o.start()

    c_m1(0).start()
    normalise(1)
    c_p1(2).start()
    normalise(3)
    c_m1(1).start()
    c_p1(3).start()
    racc[...] = jnp.full(racc.shape, -1.0, F32)
    cacc[...] = jnp.full(cacc.shape, -1.0, F32)
    for j in (2, 3):
        c_m1(j).start()
        c_p1(j - 2).start()
    for j in range(NC):
        c_oo(j, c).start()

    def order_wait(slot):
        order_copy(0, slot, dev(0, x, co)).wait_recv()

    order_wait(VO + co)
    for slot in range(VP1, NV):
        order_wait(slot)

    def build_rows(slot, v):
        for j in range(NC):
            line = ordv[v, pl.ds(j, 1)].astype(F32)
            oa[slot, pl.ds(j * ch, ch)] = jnp.broadcast_to(line, (128, ch)).T

    build_rows(SO, VO + c)
    build_rows(SP1, VP1)
    build_rows(SM1, VM1)
    build_rows(SM2, VM2)
    build_rows(SP2, VP2 + c)
    xj = jnp.where(upper, 2, 0)
    for base, v, count, off in ((BO, VO, NC, 0), (BX1, VX1, NC, 0), (BP2, VP2, NC, 0), (BXH, VXH, 2, xj)):
        for j in range(count):
            for h in (0, 1):
                line = ordv[v + h, pl.ds(j + off, 1)].astype(F32)
                ob[base + j, :, h * ch : (h + 1) * ch] = jnp.broadcast_to(line, (8, ch))

    def tiles(a, slot, r0, nrows, tile, ntiles, with_columns=True):
        b = bbuf[pl.ds(tile, ntiles)].reshape(ntiles * 2 * ch, bbuf.shape[2])
        s = lax.dot_general(a, b, (((1,), (1,)), ((), ())), preferred_element_type=F32)
        r_sl = pl.ds(pl.multiple_of(r0, ch), nrows)
        o_rows = oa[slot, r_sl]
        best = racc[slot, r_sl]
        for t in range(ntiles):
            for h in (0, 1):
                k = t * 2 + h
                sk = s[:, k * ch : (k + 1) * ch]
                m = ob[tile + t, 0:1, h * ch : (h + 1) * ch] < o_rows
                best = jnp.maximum(best, jnp.where(m, sk, -1.0))
                if with_columns:
                    down = jnp.where(m, -1.0, sk).reshape(nrows // 8, 8, ch)
                    lanes = pl.ds(h * ch, ch)
                    cacc[tile + t, :, lanes] = jnp.maximum(cacc[tile + t, :, lanes], jnp.max(down, axis=0))
        racc[slot, r_sl] = best

    nrow = NC * ch

    def whole(slot, tile, with_columns=True):
        tiles(abuf[slot], slot, 0, nrow, tile, 1, with_columns)

    def first(k, _):
        jp = lax.rem(k + 2, NC)
        c_m1(k).wait_recv()
        c_m2(k).start()
        c_p1(jp).wait_recv()
        c_p2(jp).start()
        c_x1(jp).start()
        c_oo(k, co).wait_recv()
        whole(SO, BO + k, False)

        @pl.when(k >= 1)
        def _():
            jq = lax.rem(k + 1, NC)
            c_x1(jq).wait_recv()
            c_fwd(DX1O, BX1, jq, c).start()

        return 0

    lax.fori_loop(0, NC, first, 0)
    c_x1(1).wait_recv()
    c_fwd(DX1O, BX1, 1, c).start()

    def x1_step(i, _):
        j = lax.rem(i + 2, NC)
        c_fwd(DX1O, BX1, j, co).wait_recv()

        def one(slot, _):
            whole(slot, BX1 + j)
            return 0

        lax.fori_loop(SO, SM1 + 1, one, 0)
        return 0

    lax.fori_loop(0, NC, x1_step, 0)

    def second(k, _):
        jp = lax.rem(k + 2, NC)
        c_m2(k).wait_recv()
        c_p2(jp).wait_recv()
        c_fwd(DP2O, BP2, jp, c).start()

        @pl.when(jnp.logical_and(k < 2, upper))
        def _():
            c_xh_p(k).start()

        @pl.when(jnp.logical_and(k < 2, jnp.logical_not(upper)))
        def _():
            c_xh_m(k).start()

        tiles(rows(SM2, k)[...], SM2, k * ch, ch, BX1, NC)
        c_fwd(DP2O, BP2, jp, co).wait_recv()

        def one(slot, _):
            whole(slot, BP2 + jp)
            return 0

        lax.fori_loop(SO, SM1 + 1, one, 0)

        @pl.when(lax.rem(k, 2) == 1)
        def _():
            rm = jnp.where(jnp.logical_and(k == 3, low), 2, 0)
            bp = jnp.where(jnp.logical_and(k == 3, jnp.logical_not(low)), 0, 2)

            def one(t, _):
                r0 = pl.multiple_of(rm * ch, ch)
                tiles(abuf[SM2, pl.ds(r0, 2 * ch)], SM2, r0, 2 * ch, BP2 + bp + t, 1)
                return 0

            lax.fori_loop(0, 2, one, 0)

        @pl.when(jnp.logical_or(k == 1, k == 2))
        def _():
            c_xh_m(k - 1).wait_recv()
            c_fwd(DXHO, BXH, k - 1, c).start()

        @pl.when(k == 2)
        def _():
            for i in (0, 1):
                c_fwd(DXHO, BXH, i, co).wait_recv()

        @pl.when(k >= 2)
        def _():
            @pl.when(upper)
            def _():
                r0 = pl.multiple_of((k - 2) * 2 * ch, ch)
                tiles(abuf[SM2, pl.ds(r0, 2 * ch)], SM2, r0, 2 * ch, BXH, 2)

            @pl.when(jnp.logical_not(upper))
            def _():
                def one(t, _):
                    j = lax.rem(2 * k + 2 + t, NC)
                    tiles(half(BP2 + j, c)[...], SP2, j * ch, ch, BXH, 2)
                    return 0

                lax.fori_loop(0, 2, one, 0)

        return 0

    lax.fori_loop(0, NC, second, 0)

    def row_line(slot, j):
        return jnp.max(racc[slot, pl.ds(j * ch, ch)].T, axis=0, keepdims=True)

    def col_line(tile, h):
        return jnp.max(cacc[tile, :, h * ch : (h + 1) * ch], axis=0, keepdims=True)

    res[...] = jnp.full(res.shape, -1.0, F32)
    for j in range(NC):
        res[RM2, j : j + 1] = row_line(SM2, j)
        res[RP1, j : j + 1] = row_line(SP1, j)
        res[RM1, j : j + 1] = row_line(SM1, j)
        for h in (0, 1):
            extra = jnp.where(c == h, row_line(SP2, j), -1.0)
            res[RP2 + h, j : j + 1] = jnp.maximum(col_line(BP2 + j, h), extra)
            res[RX1 + h, j : j + 1] = col_line(BX1 + j, h)
    for h in (0, 1):
        for i in (0, 1):
            res[RXHM + h, pl.ds(xj + i, 1)] = col_line(BXH + i, h)

    def result_copy(src, dst, target):
        return pltpu.make_async_remote_copy(
            src_ref=res.at[src], dst_ref=resin.at[dst], send_sem=rsend_sem.at[src], recv_sem=rrecv_sem.at[dst],
            device_id=target, device_id_type=MESH,
        )

    sends = []
    for h in (0, 1):
        sends += [result_copy(RP2 + h, RP2 + c, dev(2, x, h)), result_copy(RX1 + h, RX1 + c, dev(1, xo, h))]
    sends += [
        result_copy(RM2, RM2, dev(-2, x, c)), result_copy(RP1, RP1, dev(1, x, c)), result_copy(RM1, RM1, dev(-1, x, c))
    ]
    for s in sends:
        s.start()

    @pl.when(upper)
    def _():
        for h in (0, 1):
            result_copy(RXHM + h, RXHP + c, dev(2, xo, h)).start()

    @pl.when(jnp.logical_not(upper))
    def _():
        for h in (0, 1):
            result_copy(RXHM + h, RXHM + c, dev(-2, xo, h)).start()

    for j in range(NC):
        fin[j : j + 1] = row_line(SO, j)

    def sent(j, _):
        for copy in (c_m1, c_p1, c_m2, c_p2, c_x1):
            copy(j).wait_send()
        c_oo(j, c).wait_send()
        c_fwd(DP2O, BP2, j, c).wait_send()
        c_fwd(DX1O, BX1, j, c).wait_send()
        return 0

    lax.fori_loop(0, NC, sent, 0)
    for i in (0, 1):
        c_xh_m(i).wait_send()
        c_fwd(DXHO, BXH, i, c).wait_send()
    for o in order_sends:
        o.wait_send()

    @pl.when(low)
    def _():
        for o in order_sends_low:
            o.wait_send()

    for slot in range(RXHM):
        result_copy(0, slot, dev(1, x, c)).wait_recv()
        fin[...] = jnp.maximum(fin[...], resin[slot])

    @pl.when(low)
    def _():
        for slot in range(RXHM, NR):
            result_copy(0, slot, dev(1, x, c)).wait_recv()
            fin[...] = jnp.maximum(fin[...], resin[slot])

    for src in range(RXHM + 2):
        result_copy(src, 0, dev(1, x, c)).wait_send()
    best = fin[...]
    out_ref[0] = best
    out_ref[1] = jnp.maximum(best - thr_ref[0], 0.0)


def shards(embeddings, member_order, threshold):
    r, e = embeddings.shape
    ch = r // NC
    out = pl.pallas_call(
        kernel,
        out_shape=jax.ShapeDtypeStruct((2, NC, ch), F32),
        in_specs=[
            pl.BlockSpec(memory_space=pltpu.VMEM),
            pl.BlockSpec(memory_space=pltpu.SMEM),
            pl.BlockSpec(memory_space=pl.ANY),
        ],
        out_specs=pl.BlockSpec(memory_space=pltpu.VMEM),
        scratch_shapes=[
            pltpu.VMEM((NC, ch, e), F32),
            pltpu.VMEM((4, r, e), BF16),
            pltpu.VMEM((NB, 2 * ch, e), BF16),
            pltpu.VMEM((5, r, ch), F32),
            pltpu.VMEM((NB, 8, 2 * ch), F32),
            pltpu.VMEM((5, r, ch), F32),
            pltpu.VMEM((NB, 8, 2 * ch), F32),
            pltpu.VMEM((NV, NC, ch), jnp.int32),
            pltpu.VMEM((RXHM + 2, NC, ch), F32),
            pltpu.VMEM((NR, NC, ch), F32),
            pltpu.VMEM((NC, ch), F32),
            pltpu.SemaphoreType.DMA((NC,)),
            pltpu.SemaphoreType.DMA((ND, NC)),
            pltpu.SemaphoreType.DMA((ND, NC)),
            pltpu.SemaphoreType.DMA((12,)),
            pltpu.SemaphoreType.DMA((NV,)),
            pltpu.SemaphoreType.DMA((RXHM + 2,)),
            pltpu.SemaphoreType.DMA((NR,)),
        ],
        compiler_params=pltpu.CompilerParams(
            collective_id=0, has_side_effects=True, vmem_limit_bytes=60 * 1024 * 1024
        ),
    )(member_order.reshape(NC, ch), threshold, embeddings)
    return out[0].reshape(r), out[1].reshape(r)


def solution(mesh):
    placed = (P(("clusters", "members"), None), P(("clusters", "members")), P("clusters"))
    return jax.shard_map(
        shards,
        mesh=mesh,
        in_specs=placed,
        out_specs=(P(("clusters", "members")), P(("clusters", "members"))),
        check_vma=False,
    )
```

```python
import jax
import jax.numpy as jnp
from jax import lax
from jax.experimental import pallas as pl
from jax.experimental.pallas import tpu as pltpu
from jax.sharding import PartitionSpec as P

MESH = pl.DeviceIdType.MESH
F32 = jnp.float32
BF16 = jnp.bfloat16

SO, SP1, SM1, SM2, SP2, NS = range(6)
BO, BP1, BX1, BP2, BXH, NB = 0, 4, 8, 12, 16, 18
DM1, DP1, DOO, DM2, DP2, DX1, DXH, DP1O, DX1O, DP2O, DXHO, ND = range(12)
VO, VP1, VM1, VM2, VP2, VX1, VXH, NV = 0, 2, 4, 5, 6, 8, 10, 12
RP1, RM1, RM2, RP2, RX1, RXHM, RXHP, NR = 0, 2, 3, 4, 6, 8, 10, 12
NSRC = RXHM + 2
LANES = 128
NT = 4
SUB = 1
NC = NT * SUB


def kernel(
    order_hbm, thr_hbm, emb_ref, out_ref,
    order_ref, thr_ref, stage, abuf, bbuf, racc, cacc, oa, ob, ordv, res, resin,
    load_sem, small_sem, send_sem, recv_sem, osend_sem, orecv_sem, rsend_sem, rrecv_sem,
):
    n = lax.axis_size("members")
    nz = n // 4
    me = lax.axis_index("members")
    z, x, c = lax.div(me, 4), lax.rem(lax.div(me, 2), 2), lax.rem(me, 2)
    xo, co = 1 - x, 1 - c
    ch = abuf.shape[1] // NC

    def dev(dz, px, pc):
        return {"members": lax.rem(z + dz + nz, nz) * 4 + px * 2 + pc}

    upper = lax.rem(z + 2, nz) < nz // 2
    low = z < nz // 2

    loads = [
        pltpu.make_async_copy(emb_ref.at[pl.ds(j * ch, ch)], stage.at[j], load_sem.at[j]) for j in range(NC)
    ]
    order_in = [j + s for j in range(NC // 2) for s in (0, NC // 2)]
    for j in order_in:
        loads[j].start()
    order_load = pltpu.make_async_copy(order_hbm, order_ref, small_sem.at[0])
    order_load.start()
    thr_load = pltpu.make_async_copy(thr_hbm, thr_ref, small_sem.at[1])
    thr_load.start()

    peers = [dev(0, x, co), dev(0, xo, c)]
    for h in (0, 1):
        for dz in (2, -2, 1, -1):
            peers += [dev(dz, xo, h), dev(dz, x, h)]
    barrier = pltpu.get_barrier_semaphore()
    for p in peers:
        pl.semaphore_signal(barrier, inc=1, device_id=p, device_id_type=MESH)

    def remote(kind, j, src, dst, target):
        return pltpu.make_async_remote_copy(
            src_ref=src, dst_ref=dst, send_sem=send_sem.at[kind, j], recv_sem=recv_sem.at[kind, j],
            device_id=target, device_id_type=MESH,
        )

    def rows(slot, j):
        return abuf.at[slot, pl.ds(pl.multiple_of(j * ch, ch), ch)]

    def half(base, j, h):
        return bbuf.at[base + lax.div(j, SUB), pl.ds(pl.multiple_of(h * LANES + lax.rem(j, SUB) * ch, ch), ch)]

    def c_m1(j):
        return remote(DM1, j, rows(SO, j), rows(SM1, j), dev(1, x, c))

    def c_p1(j):
        return remote(DP1, j, rows(SO, j), rows(SP1, j), dev(-1, x, c))

    def c_m2(j):
        return remote(DM2, j, rows(SM1, j), rows(SM2, j), dev(1, x, c))

    def c_p2(j):
        return remote(DP2, j, rows(SP1, j), half(BP2, j, c), dev(-1, x, c))

    def c_x1(j):
        return remote(DX1, j, rows(SP1, j), half(BX1, j, c), dev(0, xo, c))

    def c_xh_m(i):
        return remote(DXH, i, rows(SM2, i), half(BXH, i, c), dev(0, xo, c))

    def c_xh_p(i):
        return remote(DXH, i, half(BP2, NC // 2 + i, c), half(BXH, i, c), dev(0, xo, c))

    def c_oo(j, h):
        return remote(DOO, j, rows(SO, j), half(BO, j, h), dev(0, x, co))

    def c_p1o(j, h):
        return remote(DP1O, j, rows(SP1, j), half(BP1, j, h), dev(0, x, co))

    def c_fwd(kind, base, j, h):
        return remote(kind, j, half(base, j, h), half(base, j, h), dev(0, x, co))

    def normalise(j):
        loads[j].wait()
        e = stage[j]
        u = (e * lax.rsqrt(jnp.sum(e * e, axis=1, keepdims=True) + 1e-06)).astype(BF16)
        abuf[SO, pl.ds(j * ch, ch)] = u
        bbuf[BO + j // SUB, pl.ds(pl.multiple_of(c * LANES + (j % SUB) * ch, ch), ch)] = u

    normalise(0)
    order_load.wait()
    ordv[c] = order_ref[...]
    pl.semaphore_wait(barrier, len(peers))
    def order_copy(k, slot, target):
        return pltpu.make_async_remote_copy(
            src_ref=order_ref, dst_ref=ordv.at[slot], send_sem=osend_sem.at[k], recv_sem=orecv_sem.at[slot],
            device_id=target, device_id_type=MESH,
        )

    order_sends = [order_copy(0, VO + c, dev(0, x, co)), order_copy(1, VM1, dev(1, x, c)), order_copy(2, VM2, dev(2, x, c))]
    order_sends_low = []
    for h in (0, 1):
        order_sends += [
            order_copy(3 + h, VP1 + c, dev(-1, x, h)), order_copy(5 + h, VP2 + c, dev(-2, x, h)),
            order_copy(7 + h, VX1 + c, dev(-1, xo, h)),
        ]
        order_sends_low += [order_copy(9 + h, VXH + c, dev(2, xo, h)), order_copy(11 + h, VXH + c, dev(-2, xo, h))]
    for o in order_sends:
        o.start()

    @pl.when(low)
    def _():
        for o in order_sends_low:
            o.start()

    for i in range(NC // 2):
        c_m1(i).start()
        normalise(NC // 2 + i)
        if i + 1 < NC // 2:
            normalise(i + 1)
        c_p1(NC // 2 + i).start()
    for i in range(NC // 2):
        c_m1(NC // 2 + i).start()
        c_p1(i).start()

    for j in range(NC):
        c_oo(j, c).start()
    racc[...] = jnp.full(racc.shape, -1.0, F32)
    cacc[...] = jnp.full(cacc.shape, -1.0, F32)
    res[...] = jnp.full(res.shape, -1.0, F32)

    def order_wait(slot):
        order_copy(0, slot, dev(0, x, co)).wait_recv()

    order_wait(VO + co)
    for slot in range(VP1, NV):
        order_wait(slot)

    for slot, v in ((SO, VO + c), (SP1, VP1 + c), (SM1, VM1), (SM2, VM2), (SP2, VP2 + c)):
        for j in range(NT):
            line = ordv[v, pl.ds(j, 1)].astype(F32)
            oa[slot, pl.ds(j * LANES, LANES)] = jnp.broadcast_to(line, (LANES, LANES)).T
    xj = jnp.where(upper, 2, 0)
    for base, v, count, off in ((BO, VO, NT, 0), (BP1, VP1, NT, 0), (BX1, VX1, NT, 0), (BP2, VP2, NT, 0), (BXH, VXH, 2, xj)):
        for j in range(count):
            for h in (0, 1):
                line = ordv[v + h, pl.ds(j + off, 1)].astype(F32)
                ob[base + j, :, h * LANES : (h + 1) * LANES] = jnp.broadcast_to(line, (8, LANES))

    def tiles(slot, r0, nrows, tile, ntiles, with_columns=True):
        r_sl = pl.ds(r0, nrows) if isinstance(r0, int) else pl.ds(pl.multiple_of(r0, LANES), nrows)
        b = bbuf[pl.ds(tile, ntiles)].reshape(ntiles * 2 * LANES, bbuf.shape[2])
        s = lax.dot_general(abuf[slot, r_sl], b, (((1,), (1,)), ((), ())), preferred_element_type=F32)
        o_rows = oa[slot, r_sl]
        best = racc[slot, r_sl]
        for t in range(ntiles):
            for h in (0, 1):
                k = t * 2 + h
                sk = s[:, k * LANES : (k + 1) * LANES]
                m = ob[tile + t, 0:1, h * LANES : (h + 1) * LANES] < o_rows
                best = jnp.maximum(best, jnp.where(m, sk, -1.0))
                if with_columns:
                    down = jnp.where(m, -1.0, sk).reshape(nrows // 8, 8, LANES)
                    lanes = pl.ds(h * LANES, LANES)
                    cacc[tile + t, :, lanes] = jnp.maximum(cacc[tile + t, :, lanes], jnp.max(down, axis=0))
        racc[slot, r_sl] = best

    nrow = NT * LANES
    two = 2 * LANES

    def whole(slot, tile, with_columns=True):
        tiles(slot, 0, nrow, tile, 1, with_columns)

    def loop(lo, hi, body):
        def step(i, _):
            body(i)
            return 0

        lax.fori_loop(lo, hi, step, 0)

    def turned(t):
        return lax.rem(t + NT // 2, NT)

    def subs(t):
        return [SUB * t + i for i in range(SUB)]

    def first_step(k):
        jp = lax.rem(k + NC // 2, NC)
        c_m1(k).wait_recv()
        c_m2(k).start()
        c_p1(jp).wait_recv()
        c_p2(jp).start()
        c_x1(jp).start()
        c_p1o(jp, c).start()
        half(BP1, jp, c)[...] = rows(SP1, jp)[...]

    def x1_forward(t):
        for j in subs(turned(t)):
            c_x1(j).wait_recv()
            c_fwd(DX1O, BX1, j, c).start()

    def x1_ready(t):
        for j in subs(turned(t)):
            c_fwd(DX1O, BX1, j, co).wait_recv()

    def p1_own(t):
        for j in subs(turned(t)):
            c_p1o(j, co).wait_recv()
        whole(SO, BP1 + turned(t))

    def first(kk):
        for k in subs(kk)[: max(SUB // 2, 1)]:
            first_step(k)
        for j in subs(kk):
            c_oo(j, co).wait_recv()
        whole(SO, BO + kk, False)

        @pl.when(kk >= 1)
        def _():
            p1_own(kk - 1)

        for k in subs(kk)[max(SUB // 2, 1) :]:
            first_step(k)

        @pl.when(kk >= 1)
        def _():
            x1_forward(kk - 1)

        @pl.when(kk >= 2)
        def _():
            x1_ready(kk - 2)
            whole(SO, BX1 + turned(kk - 2))

    loop(0, NT, first)
    p1_own(NT - 1)
    loop(0, NT, lambda t: whole(SM1, BP1 + t))

    def second_step(k):
        jp = lax.rem(k + NC // 2, NC)
        c_m2(k).wait_recv()
        c_p2(jp).wait_recv()
        c_fwd(DP2O, BP2, jp, c).start()

        @pl.when(jnp.logical_and(k < NC // 2, upper))
        def _():
            c_xh_p(k).start()

        @pl.when(jnp.logical_and(k < NC // 2, jnp.logical_not(upper)))
        def _():
            c_xh_m(k).start()

        rows(SP2, jp)[...] = half(BP2, jp, c)[...]

    def half_rows(q):
        slot = jnp.where(upper, SM2, SP2)
        tiles(slot, jnp.where(upper, q, 1 - q) * two, two, BXH, 2)

    def row_line(slot, j):
        return jnp.max(racc[slot, pl.ds(j * LANES, LANES)].T, axis=0, keepdims=True)

    def col_line(tile, h):
        return jnp.max(cacc[tile, :, h * LANES : (h + 1) * LANES], axis=0, keepdims=True)

    def result_copy(src, dst, target):
        return pltpu.make_async_remote_copy(
            src_ref=res.at[src], dst_ref=resin.at[dst], send_sem=rsend_sem.at[src], recv_sem=rrecv_sem.at[dst],
            device_id=target, device_id_type=MESH,
        )

    def both_halves(dst, base, slot):
        for j in range(NT):
            line = row_line(slot, j)
            for h in (0, 1):
                res[dst + h, j : j + 1] = jnp.maximum(col_line(base + j, h), jnp.where(c == h, line, -1.0))

    def second(kk):
        for k in subs(kk)[: max(SUB // 2, 1)]:
            second_step(k)

        @pl.when(kk == 0)
        def _():
            x1_ready(2)
            whole(SO, BX1 + turned(2))

            def one(i):
                whole(SP1 + lax.rem(i, 2), BX1 + turned(lax.div(i, 2)))

            loop(0, 4, one)

        @pl.when(kk == 1)
        def _():
            x1_ready(3)
            loop(SO, SM1 + 1, lambda s: whole(s, BX1 + turned(3)))

        @pl.when(kk == 2)
        def _():
            both_halves(RP1, BP1, SP1)

        @pl.when(kk == 3)
        def _():
            for h in (0, 1):
                result_copy(RP1 + h, RP1 + c, dev(1, x, h)).start()
            for i in range(NC // 2):
                c_fwd(DXHO, BXH, i, co).wait_recv()
            half_rows(0)

        for k in subs(kk)[max(SUB // 2, 1) :]:
            second_step(k)

        @pl.when(kk == 0)
        def _():
            x1_forward(3)
            loop(SP1, SM1 + 1, lambda s: whole(s, BX1 + turned(2)))

        @pl.when(jnp.logical_or(kk == 1, kk == 2))
        def _():
            for i in subs(kk - 1):
                c_xh_m(i).wait_recv()
                c_fwd(DXHO, BXH, i, c).start()

        @pl.when(lax.rem(kk, 2) == 1)
        def _():
            tiles(SM2, (kk - 1) * LANES, two, BX1, NT)

        for j in subs(turned(kk)):
            c_fwd(DP2O, BP2, j, co).wait_recv()
        whole(SM1, BP2 + turned(kk))

        @pl.when(lax.rem(kk, 2) == 1)
        def _():
            last = kk == 3
            rm = jnp.where(jnp.logical_and(last, low), two, 0)
            bp = jnp.where(jnp.logical_and(last, jnp.logical_not(low)), 0, 2)
            tiles(SM2, rm, two, BP2 + bp, 2)

    loop(0, NT, second)
    half_rows(1)

    for j in range(NT):
        res[RM2, j : j + 1] = row_line(SM2, j)
    both_halves(RP2, BP2, SP2)
    for j in range(NT):
        for h in (0, 1):
            res[RX1 + h, j : j + 1] = col_line(BX1 + j, h)
        res[RM1, j : j + 1] = row_line(SM1, j)
    for h in (0, 1):
        for i in (0, 1):
            res[RXHM + h, pl.ds(xj + i, 1)] = col_line(BXH + i, h)

    result_copy(RM2, RM2, dev(-2, x, c)).start()
    for h in (0, 1):
        result_copy(RP2 + h, RP2 + c, dev(2, x, h)).start()
        result_copy(RX1 + h, RX1 + c, dev(1, xo, h)).start()

    @pl.when(upper)
    def _():
        for h in (0, 1):
            result_copy(RXHM + h, RXHP + c, dev(2, xo, h)).start()

    @pl.when(jnp.logical_not(upper))
    def _():
        for h in (0, 1):
            result_copy(RXHM + h, RXHM + c, dev(-2, xo, h)).start()

    result_copy(RM1, RM1, dev(-1, x, c)).start()

    for j in range(NT):
        out_ref[0, j : j + 1] = row_line(SO, j)

    def sent(j):
        for copy in (c_m1, c_p1, c_m2, c_p2, c_x1):
            copy(j).wait_send()
        c_oo(j, c).wait_send()
        c_p1o(j, c).wait_send()
        c_fwd(DP2O, BP2, j, c).wait_send()
        c_fwd(DX1O, BX1, j, c).wait_send()

    loop(0, NC, sent)
    for i in range(NC // 2):
        c_xh_m(i).wait_send()
        c_fwd(DXHO, BXH, i, c).wait_send()
    for o in order_sends:
        o.wait_send()

    @pl.when(low)
    def _():
        for o in order_sends_low:
            o.wait_send()

    for slot in range(RXHM):
        result_copy(0, slot, dev(1, x, c)).wait_recv()
    thr_load.wait()
    best = out_ref[0]
    for slot in range(RXHM):
        best = jnp.maximum(best, resin[slot])
    out_ref[0] = best
    out_ref[1] = jnp.maximum(best - thr_ref[...], 0.0)

    @pl.when(low)
    def _():
        for slot in range(RXHM, NR):
            result_copy(0, slot, dev(1, x, c)).wait_recv()
        more = out_ref[0]
        for slot in range(RXHM, NR):
            more = jnp.maximum(more, resin[slot])
        out_ref[0] = more
        out_ref[1] = jnp.maximum(more - thr_ref[...], 0.0)

    for src in range(NSRC):
        result_copy(src, 0, dev(1, x, c)).wait_send()


def shards(embeddings, member_order, threshold):
    r, e = embeddings.shape
    out = pl.pallas_call(
        kernel,
        out_shape=jax.ShapeDtypeStruct((2, NT, LANES), F32),
        in_specs=[pl.BlockSpec(memory_space=pl.ANY)] * 3,
        out_specs=pl.BlockSpec(memory_space=pltpu.VMEM),
        scratch_shapes=[
            pltpu.VMEM((NT, LANES), jnp.int32),
            pltpu.VMEM((1, 1), F32),
            pltpu.VMEM((NC, r // NC, e), F32),
            pltpu.VMEM((NS, r, e), BF16),
            pltpu.VMEM((NB, 2 * LANES, e), BF16),
            pltpu.VMEM((NS, r, LANES), F32),
            pltpu.VMEM((NB, 8, 2 * LANES), F32),
            pltpu.VMEM((NS, r, LANES), F32),
            pltpu.VMEM((NB, 8, 2 * LANES), F32),
            pltpu.VMEM((NV, NT, LANES), jnp.int32),
            pltpu.VMEM((NSRC, NT, LANES), F32),
            pltpu.VMEM((NR, NT, LANES), F32),
            pltpu.SemaphoreType.DMA((NC,)),
            pltpu.SemaphoreType.DMA((2,)),
            pltpu.SemaphoreType.DMA((ND, NC)),
            pltpu.SemaphoreType.DMA((ND, NC)),
            pltpu.SemaphoreType.DMA((13,)),
            pltpu.SemaphoreType.DMA((NV,)),
            pltpu.SemaphoreType.DMA((NSRC,)),
            pltpu.SemaphoreType.DMA((NR,)),
        ],
        compiler_params=pltpu.CompilerParams(
            collective_id=0, has_side_effects=True, vmem_limit_bytes=52 * 1024 * 1024
        ),
    )(member_order.reshape(NT, LANES), threshold.reshape(1, 1), embeddings)
    return out[0].reshape(r), out[1].reshape(r)


def solution(mesh):
    placed = (P(("clusters", "members"), None), P(("clusters", "members")), P("clusters"))
    return jax.shard_map(
        shards,
        mesh=mesh,
        in_specs=placed,
        out_specs=(P(("clusters", "members")), P(("clusters", "members"))),
        check_vma=False,
    )
```

```python
import jax
import jax.numpy as jnp
from jax import lax
from jax.experimental import pallas as pl
from jax.experimental.pallas import tpu as pltpu
from jax.sharding import PartitionSpec as P

MESH = pl.DeviceIdType.MESH
F32 = jnp.float32
BF16 = jnp.bfloat16

SO, SP1, SM1, SM2, SP2, NS = range(6)
BO, BP1, BX1, BP2, BXH, NB = 0, 4, 8, 12, 16, 18
DM1, DP1, DM2, DP2, DX1, DP1O, DX1O, DP2O, DXH, DOO, DXHO, ND = range(12)
VO, VP1, VM1, VM2, VP2, VX1, VXH, NV = 0, 2, 4, 5, 6, 8, 10, 12
RP1, RM1, RM2, RP2, RX1, RXHM, RXHP, NR = 0, 2, 3, 4, 6, 8, 10, 12
NSRC = RXHM + 2
LANES = 128
NT = 4
SUB = 1
NC = NT * SUB


def kernel(
    order_hbm, thr_hbm, emb_ref, out_ref,
    order_ref, thr_ref, stage, abuf, bbuf, racc, cacc, oa, ob, ordv, res, resin,
    load_sem, small_sem, send_sem, recv_sem, vec_sem, orecv_sem,
):
    n = lax.axis_size("members")
    nz = n // 4
    me = lax.axis_index("members")
    z, x, c = lax.div(me, 4), lax.rem(lax.div(me, 2), 2), lax.rem(me, 2)
    xo, co = 1 - x, 1 - c
    ch = abuf.shape[1] // NC

    def dev(dz, px, pc):
        return {"members": lax.rem(z + dz + nz, nz) * 4 + px * 2 + pc}

    upper = lax.rem(z + 2, nz) < nz // 2
    low = z < nz // 2

    loads = [
        pltpu.make_async_copy(emb_ref.at[pl.ds(j * ch, ch)], stage.at[j], load_sem.at[j]) for j in range(NC)
    ]
    order_in = [j + s for j in range(NC // 2) for s in (0, NC // 2)]
    for j in order_in:
        loads[j].start()
    order_load = pltpu.make_async_copy(order_hbm, order_ref, small_sem.at[0])
    order_load.start()
    thr_load = pltpu.make_async_copy(thr_hbm, thr_ref, small_sem.at[1])
    thr_load.start()

    peers = [dev(0, xo, c), dev(1, x, c), dev(-1, x, c), dev(0, x, co)]
    barrier = pltpu.get_barrier_semaphore()
    for p in peers:
        pl.semaphore_signal(barrier, inc=1, device_id=p, device_id_type=MESH)

    def remote(kind, j, src, dst, target):
        at = kind * NC + j if kind <= DXH else DXH * NC + NC // 2 + kind - DOO
        return pltpu.make_async_remote_copy(
            src_ref=src, dst_ref=dst, send_sem=send_sem.at[kind], recv_sem=recv_sem.at[at],
            device_id=target, device_id_type=MESH,
        )

    def all_of(kind, count):
        some = abuf.at[SO, pl.ds(0, count * ch)]
        return remote(kind, 0, some, some, dev(0, x, co))

    def rows(slot, j):
        return abuf.at[slot, pl.ds(pl.multiple_of(j * ch, ch), ch)]

    def half(base, j, h):
        return bbuf.at[base + lax.div(j, SUB), pl.ds(pl.multiple_of(h * LANES + lax.rem(j, SUB) * ch, ch), ch)]

    def c_m1(j):
        return remote(DM1, j, rows(SO, j), rows(SM1, j), dev(1, x, c))

    def c_p1(j):
        return remote(DP1, j, rows(SO, j), rows(SP1, j), dev(-1, x, c))

    def c_m2(j):
        return remote(DM2, j, rows(SM1, j), rows(SM2, j), dev(1, x, c))

    def c_p2(j):
        return remote(DP2, j, rows(SP1, j), half(BP2, j, c), dev(-1, x, c))

    def c_x1(j):
        return remote(DX1, j, rows(SP1, j), half(BX1, j, c), dev(0, xo, c))

    def c_xh_m(i):
        return remote(DXH, i, rows(SM2, i), half(BXH, i, c), dev(0, xo, c))

    def c_xh_p(i):
        return remote(DXH, i, half(BP2, NC // 2 + i, c), half(BXH, i, c), dev(0, xo, c))

    def c_oo(j, h):
        return remote(DOO, j, rows(SO, j), half(BO, j, h), dev(0, x, co))

    def c_p1o(j, h):
        return remote(DP1O, j, rows(SP1, j), half(BP1, j, h), dev(0, x, co))

    def c_fwd(kind, base, j, h):
        return remote(kind, j, half(base, j, h), half(base, j, h), dev(0, x, co))

    def normalise(j):
        loads[j].wait()
        e = stage[j]
        u = (e * lax.rsqrt(jnp.sum(e * e, axis=1, keepdims=True) + 1e-06)).astype(BF16)
        abuf[SO, pl.ds(j * ch, ch)] = u
        bbuf[BO + j // SUB, pl.ds(pl.multiple_of(c * LANES + (j % SUB) * ch, ch), ch)] = u

    normalise(0)
    order_load.wait()
    ordv[c] = order_ref[...]
    pl.semaphore_wait(barrier, len(peers))

    def order_copy(k, src, dst, target):
        return pltpu.make_async_remote_copy(
            src_ref=src, dst_ref=ordv.at[dst], send_sem=vec_sem.at[k], recv_sem=orecv_sem.at[dst],
            device_id=target, device_id_type=MESH,
        )

    def order_wait(slot):
        order_copy(0, order_ref, slot, dev(0, x, co)).wait_recv()

    def order_fwd(slot):
        order_copy(0, ordv.at[slot], slot, dev(0, x, co)).start()

    order_copy(0, order_ref, VM1, dev(1, x, c)).start()
    order_copy(0, order_ref, VP1 + c, dev(-1, x, c)).start()
    order_copy(0, order_ref, VO + c, dev(0, x, co)).start()
    c_m1(0).start()
    normalise(NC // 2)
    c_p1(NC // 2).start()
    for i in range(1, NC // 2):
        normalise(i)
        c_m1(i).start()
        normalise(NC // 2 + i)
        c_p1(NC // 2 + i).start()
    for i in range(NC // 2):
        c_m1(NC // 2 + i).start()
        c_p1(i).start()

    for j in range(NC):
        c_oo(j, c).start()
    racc[...] = jnp.full(racc.shape, -1.0, F32)
    cacc[...] = jnp.full(cacc.shape, -1.0, F32)
    res[...] = jnp.full(res.shape, -1.0, F32)

    order_wait(VM1)
    order_copy(0, ordv.at[VM1], VM2, dev(1, x, c)).start()
    order_wait(VP1 + c)
    order_copy(0, ordv.at[VP1 + c], VP2 + c, dev(-1, x, c)).start()
    order_copy(0, ordv.at[VP1 + c], VX1 + c, dev(0, xo, c)).start()
    order_fwd(VP1 + c)
    order_wait(VX1 + c)
    order_fwd(VX1 + c)
    for base in (VO, VP1, VX1):
        order_wait(base + co)

    def row_orders(slot, v):
        for j in range(NT):
            line = ordv[v, pl.ds(j, 1)].astype(F32)
            oa[slot, pl.ds(j * LANES, LANES)] = jnp.broadcast_to(line, (LANES, LANES)).T

    def column_orders(base, v, count=NT, off=0):
        for j in range(count):
            for h in (0, 1):
                line = ordv[v + h, pl.ds(j + off, 1)].astype(F32)
                ob[base + j, :, h * LANES : (h + 1) * LANES] = jnp.broadcast_to(line, (8, LANES))

    row_orders(SO, VO + c)
    row_orders(SP1, VP1 + c)
    row_orders(SM1, VM1)
    column_orders(BO, VO)
    column_orders(BP1, VP1)
    column_orders(BX1, VX1)
    xj = jnp.where(upper, 2, 0)

    def tiles(slot, r0, nrows, tile, ntiles, with_columns=True):
        r_sl = pl.ds(r0, nrows) if isinstance(r0, int) else pl.ds(pl.multiple_of(r0, LANES), nrows)
        b = bbuf[pl.ds(tile, ntiles)].reshape(ntiles * 2 * LANES, bbuf.shape[2])
        s = lax.dot_general(abuf[slot, r_sl], b, (((1,), (1,)), ((), ())), preferred_element_type=F32)
        o_rows = oa[slot, r_sl]
        best = racc[slot, r_sl]
        for t in range(ntiles):
            for h in (0, 1):
                k = t * 2 + h
                sk = s[:, k * LANES : (k + 1) * LANES]
                m = ob[tile + t, 0:1, h * LANES : (h + 1) * LANES] < o_rows
                best = jnp.maximum(best, jnp.where(m, sk, -1.0))
                if with_columns:
                    down = jnp.where(m, -1.0, sk).reshape(nrows // 8, 8, LANES)
                    lanes = pl.ds(h * LANES, LANES)
                    cacc[tile + t, :, lanes] = jnp.maximum(cacc[tile + t, :, lanes], jnp.max(down, axis=0))
        racc[slot, r_sl] = best

    nrow = NT * LANES
    two = 2 * LANES

    def whole(slot, tile, with_columns=True):
        tiles(slot, 0, nrow, tile, 1, with_columns)

    def loop(lo, hi, body):
        def step(i, _):
            body(i)
            return 0

        lax.fori_loop(lo, hi, step, 0)

    def turned(t):
        return lax.rem(t + NT // 2, NT)

    def subs(t):
        return [SUB * t + i for i in range(SUB)]

    def first_step(k):
        jp = lax.rem(k + NC // 2, NC)
        c_m1(k).wait_recv()
        c_m2(k).start()
        c_p1(jp).wait_recv()
        c_p2(jp).start()
        c_x1(jp).start()
        c_p1o(jp, c).start()
        half(BP1, jp, c)[...] = rows(SP1, jp)[...]

    def x1_forward(t):
        for j in subs(turned(t)):
            c_x1(j).wait_recv()
            c_fwd(DX1O, BX1, j, c).start()

    def x1_ready(t):
        for j in subs(turned(t)):
            c_fwd(DX1O, BX1, j, co).wait_recv()

    def p1_own(t):
        for j in subs(turned(t)):
            c_p1o(j, co).wait_recv()
        whole(SO, BP1 + turned(t))

    def first(kk):
        for k in subs(kk)[: max(SUB // 2, 1)]:
            first_step(k)

        @pl.when(kk == 0)
        def _():
            all_of(DOO, NC).wait_recv()

        whole(SO, BO + kk, False)

        @pl.when(kk >= 1)
        def _():
            p1_own(kk - 1)

        for k in subs(kk)[max(SUB // 2, 1) :]:
            first_step(k)

        @pl.when(kk >= 1)
        def _():
            x1_forward(kk - 1)

        @pl.when(kk >= 2)
        def _():
            x1_ready(kk - 2)
            whole(SO, BX1 + turned(kk - 2))

    loop(0, NT, first)
    p1_own(NT - 1)
    loop(0, NT, lambda t: whole(SM1, BP1 + t))

    def second_step(k):
        jp = lax.rem(k + NC // 2, NC)
        c_m2(k).wait_recv()
        c_p2(jp).wait_recv()
        c_fwd(DP2O, BP2, jp, c).start()

        @pl.when(jnp.logical_and(k < NC // 2, upper))
        def _():
            c_xh_p(k).start()

        @pl.when(jnp.logical_and(k < NC // 2, jnp.logical_not(upper)))
        def _():
            c_xh_m(k).start()

        rows(SP2, jp)[...] = half(BP2, jp, c)[...]

    def half_rows(q):
        slot = jnp.where(upper, SM2, SP2)
        tiles(slot, jnp.where(upper, q, 1 - q) * two, two, BXH, 2)

    def row_line(slot, j):
        return jnp.max(racc[slot, pl.ds(j * LANES, LANES)].T, axis=0, keepdims=True)

    def col_line(tile, h):
        return jnp.max(cacc[tile, :, h * LANES : (h + 1) * LANES], axis=0, keepdims=True)

    def result_copy(src, dst, target, k=4):
        return pltpu.make_async_remote_copy(
            src_ref=res.at[src], dst_ref=resin.at[dst], send_sem=vec_sem.at[3], recv_sem=vec_sem.at[k],
            device_id=target, device_id_type=MESH,
        )

    def both_halves(dst, base, slot):
        for j in range(NT):
            line = row_line(slot, j)
            for h in (0, 1):
                res[dst + h, j : j + 1] = jnp.maximum(col_line(base + j, h), jnp.where(c == h, line, -1.0))

    def second(kk):
        for k in subs(kk)[: max(SUB // 2, 1)]:
            second_step(k)

        @pl.when(kk == 0)
        def _():
            order_wait(VM2)
            order_wait(VP2 + c)
            order_fwd(VP2 + c)
            order_copy(0, ordv.at[jnp.where(upper, VP2 + c, VM2)], VXH + c, dev(0, xo, c)).start()
            x1_ready(2)
            whole(SO, BX1 + turned(2))

            def one(i):
                whole(SP1 + lax.rem(i, 2), BX1 + turned(lax.div(i, 2)))

            loop(0, 4, one)
            order_wait(VP2 + co)
            row_orders(SM2, VM2)
            row_orders(SP2, VP2 + c)
            column_orders(BP2, VP2)

        @pl.when(kk == 1)
        def _():
            x1_ready(3)
            loop(SO, SM1 + 1, lambda s: whole(s, BX1 + turned(3)))

        @pl.when(kk == 2)
        def _():
            both_halves(RP1, BP1, SP1)
            order_wait(VXH + c)
            order_fwd(VXH + c)

        @pl.when(kk == 3)
        def _():
            order_wait(VXH + co)
            column_orders(BXH, VXH, 2, xj)
            for h in (0, 1):
                result_copy(RP1 + h, RP1 + c, dev(1, x, h)).start()
            all_of(DXHO, NC // 2).wait_recv()
            half_rows(0)

        for k in subs(kk)[max(SUB // 2, 1) :]:
            second_step(k)

        @pl.when(kk == 0)
        def _():
            x1_forward(3)
            loop(SP1, SM1 + 1, lambda s: whole(s, BX1 + turned(2)))

        @pl.when(jnp.logical_or(kk == 1, kk == 2))
        def _():
            for i in subs(kk - 1):
                c_xh_m(i).wait_recv()
                c_fwd(DXHO, BXH, i, c).start()

        @pl.when(lax.rem(kk, 2) == 1)
        def _():
            tiles(SM2, (kk - 1) * LANES, two, BX1, NT)

        @pl.when(kk == 3)
        def _():
            half_rows(1)

        @pl.when(jnp.logical_and(kk == 3, low))
        def _():
            tiles(SM2, two, two, BP2 + 2, 2)

        for j in subs(turned(kk)):
            c_fwd(DP2O, BP2, j, co).wait_recv()
        whole(SM1, BP2 + turned(kk))

        @pl.when(jnp.logical_or(kk == 1, jnp.logical_and(kk == 3, jnp.logical_not(low))))
        def _():
            tiles(SM2, 0, two, BP2 + jnp.where(kk == 1, 2, 0), 2)

    loop(0, NT, second)

    for j in range(NT):
        res[RM2, j : j + 1] = row_line(SM2, j)
    both_halves(RP2, BP2, SP2)
    for j in range(NT):
        for h in (0, 1):
            res[RX1 + h, j : j + 1] = col_line(BX1 + j, h)
        res[RM1, j : j + 1] = row_line(SM1, j)
    for h in (0, 1):
        for i in (0, 1):
            res[RXHM + h, pl.ds(xj + i, 1)] = col_line(BXH + i, h)

    result_copy(RM2, RM2, dev(-2, x, c)).start()
    for h in (0, 1):
        result_copy(RP2 + h, RP2 + c, dev(2, x, h)).start()
        result_copy(RX1 + h, RX1 + c, dev(1, xo, h)).start()

    @pl.when(upper)
    def _():
        for h in (0, 1):
            result_copy(RXHM + h, RXHP + c, dev(2, xo, h), 5).start()

    @pl.when(jnp.logical_not(upper))
    def _():
        for h in (0, 1):
            result_copy(RXHM + h, RXHM + c, dev(-2, xo, h), 5).start()

    result_copy(RM1, RM1, dev(-1, x, c)).start()

    for j in range(NT):
        out_ref[0, j : j + 1] = row_line(SO, j)

    for kind in range(ND):
        all_of(kind, NC // 2 if kind in (DXH, DXHO) else NC).wait_send()
    some = ordv.at[pl.ds(0, 11)]
    pltpu.make_async_remote_copy(
        src_ref=some, dst_ref=some, send_sem=vec_sem.at[0], recv_sem=orecv_sem.at[0],
        device_id=dev(0, x, co), device_id_type=MESH,
    ).wait_send()
    result_copy(pl.ds(0, RXHM), pl.ds(0, RXHM), dev(1, x, c)).wait_recv()
    thr_load.wait()
    best = out_ref[0]
    for slot in range(RXHM):
        best = jnp.maximum(best, resin[slot])
    out_ref[0] = best
    out_ref[1] = jnp.maximum(best - thr_ref[...], 0.0)

    @pl.when(low)
    def _():
        result_copy(pl.ds(0, NR - RXHM), pl.ds(RXHM, NR - RXHM), dev(1, x, c), 5).wait_recv()
        more = out_ref[0]
        for slot in range(RXHM, NR):
            more = jnp.maximum(more, resin[slot])
        out_ref[0] = more
        out_ref[1] = jnp.maximum(more - thr_ref[...], 0.0)

    result_copy(pl.ds(0, NSRC), pl.ds(0, NSRC), dev(1, x, c)).wait_send()


def shards(embeddings, member_order, threshold):
    r, e = embeddings.shape
    out = pl.pallas_call(
        kernel,
        out_shape=jax.ShapeDtypeStruct((2, NT, LANES), F32),
        in_specs=[pl.BlockSpec(memory_space=pl.ANY)] * 3,
        out_specs=pl.BlockSpec(memory_space=pltpu.VMEM),
        scratch_shapes=[
            pltpu.VMEM((NT, LANES), jnp.int32),
            pltpu.VMEM((1, 1), F32),
            pltpu.VMEM((NC, r // NC, e), F32),
            pltpu.VMEM((NS, r, e), BF16),
            pltpu.VMEM((NB, 2 * LANES, e), BF16),
            pltpu.VMEM((NS, r, LANES), F32),
            pltpu.VMEM((NB, 8, 2 * LANES), F32),
            pltpu.VMEM((NS, r, LANES), F32),
            pltpu.VMEM((NB, 8, 2 * LANES), F32),
            pltpu.VMEM((NV, NT, LANES), jnp.int32),
            pltpu.VMEM((NSRC, NT, LANES), F32),
            pltpu.VMEM((NR, NT, LANES), F32),
            pltpu.SemaphoreType.DMA((NC,)),
            pltpu.SemaphoreType.DMA((2,)),
            pltpu.SemaphoreType.DMA((ND,)),
            pltpu.SemaphoreType.DMA((DXH * NC + NC // 2 + 2,)),
            pltpu.SemaphoreType.DMA((6,)),
            pltpu.SemaphoreType.DMA((NV,)),
        ],
        compiler_params=pltpu.CompilerParams(
            collective_id=0, has_side_effects=True, vmem_limit_bytes=52 * 1024 * 1024
        ),
    )(member_order.reshape(NT, LANES), threshold.reshape(1, 1), embeddings)
    return out[0].reshape(r), out[1].reshape(r)


def solution(mesh):
    placed = (P(("clusters", "members"), None), P(("clusters", "members")), P("clusters"))
    return jax.shard_map(
        shards,
        mesh=mesh,
        in_specs=placed,
        out_specs=(P(("clusters", "members")), P(("clusters", "members"))),
        check_vma=False,
    )
```

```python
import jax
import jax.numpy as jnp
from jax import lax
from jax.experimental import pallas as pl
from jax.experimental.pallas import tpu as pltpu
from jax.sharding import PartitionSpec as P

MESH = pl.DeviceIdType.MESH
F32 = jnp.float32
BF16 = jnp.bfloat16

SO, SP1, SM1, SM2, SP2, NS = range(6)
BO, BP1, BX1, BM1, BXH, BQ, NB = 0, 4, 8, 12, 16, 18, 20
DM1, DP1, DM2, DP2, DX1, DP1O, DX1O, DXH, DOO, DM1O, DXHO, DQO, ND = range(13)
VO, VP1, VM1, VM2, VP2, VX1, VXH, NV = 0, 2, 4, 6, 8, 10, 12, 14
RP1, RM1, RM2, RP2, RX1, RXHM, RXHP, NR = 0, 2, 4, 6, 8, 10, 12, 14
NSRC = RXHM + 2
LANES = 128
NT = 4
SUB = 1
NC = NT * SUB


def kernel(
    order_hbm, thr_hbm, emb_ref, out_ref,
    order_ref, thr_ref, stage, abuf, bbuf, racc, cacc, oa, ob, ordv, res, resin,
    load_sem, small_sem, send_sem, recv_sem, vec_sem, orecv_sem,
):
    n = lax.axis_size("members")
    nz = n // 4
    me = lax.axis_index("members")
    z, x, c = lax.div(me, 4), lax.rem(lax.div(me, 2), 2), lax.rem(me, 2)
    xo, co = 1 - x, 1 - c
    ch = abuf.shape[1] // NC

    def dev(dz, px, pc):
        return {"members": lax.rem(z + dz + nz, nz) * 4 + px * 2 + pc}

    upper = lax.rem(z + 2, nz) < nz // 2
    low = z < nz // 2

    loads = [
        pltpu.make_async_copy(emb_ref.at[pl.ds(j * ch, ch)], stage.at[j], load_sem.at[j]) for j in range(NC)
    ]
    order_in = [j + s for j in range(NC // 2) for s in (0, NC // 2)]
    for j in order_in:
        loads[j].start()
    order_load = pltpu.make_async_copy(order_hbm, order_ref, small_sem.at[0])
    order_load.start()
    thr_load = pltpu.make_async_copy(thr_hbm, thr_ref, small_sem.at[1])
    thr_load.start()

    peers = [dev(0, xo, c), dev(1, x, c), dev(-1, x, c), dev(0, x, co)]
    barrier = pltpu.get_barrier_semaphore()
    for p in peers:
        pl.semaphore_signal(barrier, inc=1, device_id=p, device_id_type=MESH)

    def remote(kind, j, src, dst, target):
        at = kind * NC + j if kind <= DXH else DXH * NC + NC // 2 + kind - DOO
        return pltpu.make_async_remote_copy(
            src_ref=src, dst_ref=dst, send_sem=send_sem.at[kind], recv_sem=recv_sem.at[at],
            device_id=target, device_id_type=MESH,
        )

    def all_of(kind, count):
        some = abuf.at[SO, pl.ds(0, count * ch)]
        return remote(kind, 0, some, some, dev(0, x, co))

    def rows(slot, j):
        return abuf.at[slot, pl.ds(pl.multiple_of(j * ch, ch), ch)]

    def half(base, j, h):
        return bbuf.at[base + lax.div(j, SUB), pl.ds(pl.multiple_of(h * LANES + lax.rem(j, SUB) * ch, ch), ch)]

    def c_m1(j):
        return remote(DM1, j, rows(SO, j), rows(SM1, j), dev(1, x, c))

    def c_p1(j):
        return remote(DP1, j, rows(SO, j), rows(SP1, j), dev(-1, x, c))

    def c_m2(j):
        return remote(DM2, j, rows(SM1, j), rows(SM2, j), dev(1, x, c))

    def c_p2(j):
        return remote(DP2, j, rows(SP1, j), rows(SP2, j), dev(-1, x, c))

    def c_x1(j):
        return remote(DX1, j, rows(SP1, j), half(BX1, j, c), dev(0, xo, c))

    def c_xh_m(i):
        return remote(DXH, i, rows(SM2, i), half(BXH, i, c), dev(0, xo, c))

    def c_xh_p(i):
        return remote(DXH, i, rows(SP2, NC // 2 + i), half(BXH, i, c), dev(0, xo, c))

    def c_oo(j, h):
        return remote(DOO, j, rows(SO, j), half(BO, j, h), dev(0, x, co))

    def c_p1o(j, h):
        return remote(DP1O, j, rows(SP1, j), half(BP1, j, h), dev(0, x, co))

    def c_m1o(j, h):
        return remote(DM1O, j, rows(SM1, j), half(BM1, j, h), dev(0, x, co))

    q_slot = jnp.where(low, SP2, SM2)
    q_off = jnp.where(low, NC // 2, 0)

    def c_qo(i, h):
        return remote(DQO, i, rows(q_slot, q_off + i), half(BQ, i, h), dev(0, x, co))

    def c_fwd(kind, base, j, h):
        return remote(kind, j, half(base, j, h), half(base, j, h), dev(0, x, co))

    def normalise(j):
        loads[j].wait()
        e = stage[j]
        u = (e * lax.rsqrt(jnp.sum(e * e, axis=1, keepdims=True) + 1e-06)).astype(BF16)
        abuf[SO, pl.ds(j * ch, ch)] = u
        bbuf[BO + j // SUB, pl.ds(pl.multiple_of(c * LANES + (j % SUB) * ch, ch), ch)] = u

    normalise(0)
    order_load.wait()
    ordv[c] = order_ref[...]
    pl.semaphore_wait(barrier, len(peers))

    def order_copy(k, src, dst, target):
        return pltpu.make_async_remote_copy(
            src_ref=src, dst_ref=ordv.at[dst], send_sem=vec_sem.at[k], recv_sem=orecv_sem.at[dst],
            device_id=target, device_id_type=MESH,
        )

    def order_wait(slot):
        order_copy(0, order_ref, slot, dev(0, x, co)).wait_recv()

    def order_fwd(slot):
        order_copy(0, ordv.at[slot], slot, dev(0, x, co)).start()

    order_copy(0, order_ref, VM1 + c, dev(1, x, c)).start()
    order_copy(0, order_ref, VP1 + c, dev(-1, x, c)).start()
    order_copy(0, order_ref, VO + c, dev(0, x, co)).start()
    c_m1(0).start()
    normalise(NC // 2)
    c_p1(NC // 2).start()
    for i in range(1, NC // 2):
        normalise(i)
        c_m1(i).start()
        normalise(NC // 2 + i)
        c_p1(NC // 2 + i).start()
    for i in range(NC // 2):
        c_m1(NC // 2 + i).start()
        c_p1(i).start()

    for j in range(NC):
        c_oo(j, c).start()
    racc[...] = jnp.full(racc.shape, -1.0, F32)
    cacc[...] = jnp.full(cacc.shape, -1.0, F32)
    res[...] = jnp.full(res.shape, -1.0, F32)

    order_wait(VM1 + c)
    order_copy(0, ordv.at[VM1 + c], VM2 + c, dev(1, x, c)).start()
    order_fwd(VM1 + c)
    order_wait(VP1 + c)
    order_copy(0, ordv.at[VP1 + c], VP2 + c, dev(-1, x, c)).start()
    order_copy(0, ordv.at[VP1 + c], VX1 + c, dev(0, xo, c)).start()
    order_fwd(VP1 + c)
    order_wait(VX1 + c)
    order_fwd(VX1 + c)
    for base in (VO, VP1, VM1, VX1):
        order_wait(base + co)

    def row_orders(slot, v):
        for j in range(NT):
            line = ordv[v, pl.ds(j, 1)].astype(F32)
            oa[slot, pl.ds(j * LANES, LANES)] = jnp.broadcast_to(line, (LANES, LANES)).T

    def column_orders(base, v, count=NT, off=0):
        for j in range(count):
            for h in (0, 1):
                line = ordv[v + h, pl.ds(j + off, 1)].astype(F32)
                ob[base + j, :, h * LANES : (h + 1) * LANES] = jnp.broadcast_to(line, (8, LANES))

    row_orders(SO, VO + c)
    row_orders(SP1, VP1 + c)
    row_orders(SM1, VM1 + c)
    column_orders(BM1, VM1)
    column_orders(BO, VO)
    column_orders(BP1, VP1)
    column_orders(BX1, VX1)
    xj = jnp.where(upper, 2, 0)

    def tiles(slot, r0, nrows, tile, ntiles, with_columns=True):
        r_sl = pl.ds(r0, nrows) if isinstance(r0, int) else pl.ds(pl.multiple_of(r0, LANES), nrows)
        b = bbuf[pl.ds(tile, ntiles)].reshape(ntiles * 2 * LANES, bbuf.shape[2])
        s = lax.dot_general(abuf[slot, r_sl], b, (((1,), (1,)), ((), ())), preferred_element_type=F32)
        o_rows = oa[slot, r_sl]
        best = racc[slot, r_sl]
        for t in range(ntiles):
            for h in (0, 1):
                k = t * 2 + h
                sk = s[:, k * LANES : (k + 1) * LANES]
                m = ob[tile + t, 0:1, h * LANES : (h + 1) * LANES] < o_rows
                best = jnp.maximum(best, jnp.where(m, sk, -1.0))
                if with_columns:
                    down = jnp.where(m, -1.0, sk).reshape(nrows // 8, 8, LANES)
                    lanes = pl.ds(h * LANES, LANES)
                    cacc[tile + t, :, lanes] = jnp.maximum(cacc[tile + t, :, lanes], jnp.max(down, axis=0))
        racc[slot, r_sl] = best

    nrow = NT * LANES
    two = 2 * LANES

    def whole(slot, tile, with_columns=True):
        tiles(slot, 0, nrow, tile, 1, with_columns)

    def loop(lo, hi, body):
        def step(i, _):
            body(i)
            return 0

        lax.fori_loop(lo, hi, step, 0)

    def turned(t):
        return lax.rem(t + NT // 2, NT)

    def subs(t):
        return [SUB * t + i for i in range(SUB)]

    def first_step(k):
        jp = lax.rem(k + NC // 2, NC)
        c_m1(k).wait_recv()
        c_m2(k).start()
        c_m1o(k, c).start()
        half(BM1, k, c)[...] = rows(SM1, k)[...]
        c_p1(jp).wait_recv()
        c_p2(jp).start()
        c_x1(jp).start()
        c_p1o(jp, c).start()
        half(BP1, jp, c)[...] = rows(SP1, jp)[...]

    def x1_forward(t):
        for j in subs(turned(t)):
            c_x1(j).wait_recv()
            c_fwd(DX1O, BX1, j, c).start()

    def x1_ready(t):
        for j in subs(turned(t)):
            c_fwd(DX1O, BX1, j, co).wait_recv()

    def p1_own(t):
        for j in subs(turned(t)):
            c_p1o(j, co).wait_recv()
        whole(SO, BP1 + turned(t))

    def first(kk):
        for k in subs(kk)[: max(SUB // 2, 1)]:
            first_step(k)

        @pl.when(kk == 0)
        def _():
            all_of(DOO, NC).wait_recv()

        whole(SO, BO + kk, False)

        @pl.when(kk >= 1)
        def _():
            p1_own(kk - 1)

        for k in subs(kk)[max(SUB // 2, 1) :]:
            first_step(k)

        @pl.when(kk >= 1)
        def _():
            x1_forward(kk - 1)

        @pl.when(kk >= 2)
        def _():
            x1_ready(kk - 2)
            whole(SO, BX1 + turned(kk - 2))

    loop(0, NT, first)
    p1_own(NT - 1)
    loop(0, NT, lambda t: whole(SM1, BP1 + t))

    def second_step(k):
        jp = lax.rem(k + NC // 2, NC)
        c_m2(k).wait_recv()
        c_p2(jp).wait_recv()

        @pl.when(k < NC // 2)
        def _():
            c_qo(k, c).start()
            half(BQ, k, c)[...] = rows(q_slot, q_off + k)[...]

        @pl.when(jnp.logical_and(k < NC // 2, upper))
        def _():
            c_xh_p(k).start()

        @pl.when(jnp.logical_and(k < NC // 2, jnp.logical_not(upper)))
        def _():
            c_xh_m(k).start()


    def half_rows(q):
        slot = jnp.where(upper, SM2, SP2)
        tiles(slot, jnp.where(upper, q, 1 - q) * two, two, BXH, 2)

    def q_rows(q):
        tiles(jnp.where(low, SM2, SP2), jnp.where(low, q, 1 - q) * two, two, BQ, 2)

    def row_line(slot, j):
        return jnp.max(racc[slot, pl.ds(j * LANES, LANES)].T, axis=0, keepdims=True)

    def col_line(tile, h):
        return jnp.max(cacc[tile, :, h * LANES : (h + 1) * LANES], axis=0, keepdims=True)

    def result_copy(src, dst, target, k=4):
        return pltpu.make_async_remote_copy(
            src_ref=res.at[src], dst_ref=resin.at[dst], send_sem=vec_sem.at[3], recv_sem=vec_sem.at[k],
            device_id=target, device_id_type=MESH,
        )

    def both_halves(dst, base, slot):
        for j in range(NT):
            line = row_line(slot, j)
            for h in (0, 1):
                res[dst + h, j : j + 1] = jnp.maximum(col_line(base + j, h), jnp.where(c == h, line, -1.0))

    def second(kk):
        for k in subs(kk)[: max(SUB // 2, 1)]:
            second_step(k)

        @pl.when(kk == 0)
        def _():
            order_wait(VM2 + c)
            order_wait(VP2 + c)
            order_fwd(VP2 + c)
            order_fwd(VM2 + c)
            order_copy(0, ordv.at[jnp.where(upper, VP2, VM2) + c], VXH + c, dev(0, xo, c)).start()
            x1_ready(2)
            whole(SO, BX1 + turned(2))

            def one(i):
                whole(SP1 + lax.rem(i, 2), BX1 + turned(lax.div(i, 2)))

            loop(0, 4, one)
            order_wait(VP2 + co)
            order_wait(VM2 + co)
            row_orders(SM2, VM2 + c)
            row_orders(SP2, VP2 + c)
            column_orders(BQ, jnp.where(low, VP2, VM2), 2, jnp.where(low, 2, 0))

        @pl.when(kk == 1)
        def _():
            x1_ready(3)
            loop(SO, SM1 + 1, lambda s: whole(s, BX1 + turned(3)))

        @pl.when(kk == 2)
        def _():
            both_halves(RP1, BP1, SP1)
            for j in range(NT):
                out_ref[0, j : j + 1] = row_line(SO, j)
            order_wait(VXH + c)
            order_fwd(VXH + c)

        @pl.when(kk == 3)
        def _():
            order_wait(VXH + co)
            column_orders(BXH, VXH, 2, xj)
            for h in (0, 1):
                result_copy(RP1 + h, RP1 + c, dev(1, x, h)).start()
            all_of(DXHO, NC // 2).wait_recv()
            half_rows(0)

        for k in subs(kk)[max(SUB // 2, 1) :]:
            second_step(k)

        @pl.when(kk == 0)
        def _():
            x1_forward(3)
            loop(SP1, SM1 + 1, lambda s: whole(s, BX1 + turned(2)))

        @pl.when(jnp.logical_or(kk == 1, kk == 2))
        def _():
            for i in subs(kk - 1):
                c_xh_m(i).wait_recv()
                c_fwd(DXHO, BXH, i, c).start()

        @pl.when(kk == 1)
        def _():
            all_of(DM1O, NC).wait_recv()
            all_of(DQO, NC // 2).wait_recv()
            tiles(SM2, 0, two, BX1, NT)
            tiles(SP2, two, two, BM1, NT)
            q_rows(0)

    loop(0, NT, second)

    tiles(SM2, two, two, BX1, NT)
    for h in (0, 1):
        for j in range(NT):
            res[RX1 + h, j : j + 1] = col_line(BX1 + j, h)
    half_rows(1)
    for h in (0, 1):
        result_copy(RX1 + h, RX1 + c, dev(1, xo, h)).start()
        for i in (0, 1):
            res[RXHM + h, pl.ds(xj + i, 1)] = col_line(BXH + i, h)
    tiles(SP2, 0, two, BM1, NT)

    @pl.when(upper)
    def _():
        for h in (0, 1):
            result_copy(RXHM + h, RXHP + c, dev(2, xo, h), 5).start()

    @pl.when(jnp.logical_not(upper))
    def _():
        for h in (0, 1):
            result_copy(RXHM + h, RXHM + c, dev(-2, xo, h), 5).start()

    both_halves(RM1, BM1, SM1)
    q_rows(1)
    for h in (0, 1):
        result_copy(RM1 + h, RM1 + c, dev(-1, x, h)).start()

    for j in range(NT):
        for dst, slot in ((RM2, SM2), (RP2, SP2)):
            res[dst + c, j : j + 1] = row_line(slot, j)
    for h in (0, 1):
        for i in (0, 1):
            at, line = jnp.where(low, RP2, RM2) + h, pl.ds(jnp.where(low, 2, 0) + i, 1)
            res[at, line] = jnp.maximum(res[at, line], col_line(BQ + i, h))
    for h in (0, 1):
        result_copy(RM2 + h, RM2 + c, dev(-2, x, h)).start()
        result_copy(RP2 + h, RP2 + c, dev(2, x, h)).start()

    for kind in range(ND):
        all_of(kind, NC // 2 if kind in (DXH, DXHO, DQO) else NC).wait_send()
    some = ordv.at[pl.ds(0, 13)]
    pltpu.make_async_remote_copy(
        src_ref=some, dst_ref=some, send_sem=vec_sem.at[0], recv_sem=orecv_sem.at[0],
        device_id=dev(0, x, co), device_id_type=MESH,
    ).wait_send()
    result_copy(pl.ds(0, RXHM), pl.ds(0, RXHM), dev(1, x, c)).wait_recv()
    thr_load.wait()
    best = out_ref[0]
    for slot in range(RXHM):
        best = jnp.maximum(best, resin[slot])
    out_ref[0] = best
    out_ref[1] = jnp.maximum(best - thr_ref[...], 0.0)

    @pl.when(low)
    def _():
        result_copy(pl.ds(0, NR - RXHM), pl.ds(RXHM, NR - RXHM), dev(1, x, c), 5).wait_recv()
        more = out_ref[0]
        for slot in range(RXHM, NR):
            more = jnp.maximum(more, resin[slot])
        out_ref[0] = more
        out_ref[1] = jnp.maximum(more - thr_ref[...], 0.0)

    result_copy(pl.ds(0, NSRC), pl.ds(0, NSRC), dev(1, x, c)).wait_send()


def shards(embeddings, member_order, threshold):
    r, e = embeddings.shape
    out = pl.pallas_call(
        kernel,
        out_shape=jax.ShapeDtypeStruct((2, NT, LANES), F32),
        in_specs=[pl.BlockSpec(memory_space=pl.ANY)] * 3,
        out_specs=pl.BlockSpec(memory_space=pltpu.VMEM),
        scratch_shapes=[
            pltpu.VMEM((NT, LANES), jnp.int32),
            pltpu.VMEM((1, 1), F32),
            pltpu.VMEM((NC, r // NC, e), F32),
            pltpu.VMEM((NS, r, e), BF16),
            pltpu.VMEM((NB, 2 * LANES, e), BF16),
            pltpu.VMEM((NS, r, LANES), F32),
            pltpu.VMEM((NB, 8, 2 * LANES), F32),
            pltpu.VMEM((NS, r, LANES), F32),
            pltpu.VMEM((NB, 8, 2 * LANES), F32),
            pltpu.VMEM((NV, NT, LANES), jnp.int32),
            pltpu.VMEM((NSRC, NT, LANES), F32),
            pltpu.VMEM((NR, NT, LANES), F32),
            pltpu.SemaphoreType.DMA((NC,)),
            pltpu.SemaphoreType.DMA((2,)),
            pltpu.SemaphoreType.DMA((ND,)),
            pltpu.SemaphoreType.DMA((DXH * NC + NC // 2 + ND - DOO,)),
            pltpu.SemaphoreType.DMA((6,)),
            pltpu.SemaphoreType.DMA((NV,)),
        ],
        compiler_params=pltpu.CompilerParams(
            collective_id=0, has_side_effects=True, vmem_limit_bytes=52 * 1024 * 1024
        ),
    )(member_order.reshape(NT, LANES), threshold.reshape(1, 1), embeddings)
    return out[0].reshape(r), out[1].reshape(r)


def solution(mesh):
    placed = (P(("clusters", "members"), None), P(("clusters", "members")), P("clusters"))
    return jax.shard_map(
        shards,
        mesh=mesh,
        in_specs=placed,
        out_specs=(P(("clusters", "members")), P(("clusters", "members"))),
        check_vma=False,
    )
```

```python
import jax
import jax.numpy as jnp
from jax import lax
from jax.experimental import pallas as pl
from jax.experimental.pallas import tpu as pltpu
from jax.sharding import PartitionSpec as P

MESH = pl.DeviceIdType.MESH
F32 = jnp.float32
BF16 = jnp.bfloat16

SO, SP1, SM1, SM2, SP2, NS = range(6)
BO, BP1, BX1, BM1, BXH, BQ, NB = 0, 4, 8, 12, 16, 18, 20
DM1, DP1, DM2, DP2, DX1, DP1O, DX1O, DXH, DOO, DM1O, DXHO, DQO, ND = range(13)
VO, VP1, VM1, VM2, VP2, VX1, VXH, NV = 0, 2, 4, 6, 8, 10, 12, 14
RP1, RM1, RM2, RP2, RX1, RXHM, RXHP, NR = 0, 2, 4, 6, 8, 10, 12, 14
NSRC = RXHM + 2
LANES = 128
NT = 4
SUB = 1
NC = NT * SUB


def kernel(
    order_hbm, thr_hbm, emb_ref, out_ref,
    order_ref, thr_ref, stage, abuf, bbuf, racc, cacc, oa, ob, ordv, res, resin,
    load_sem, small_sem, send_sem, recv_sem, vec_sem, orecv_sem,
):
    n = lax.axis_size("members")
    nz = n // 4
    me = lax.axis_index("members")
    z, x, c = lax.div(me, 4), lax.rem(lax.div(me, 2), 2), lax.rem(me, 2)
    xo, co = 1 - x, 1 - c
    ch = abuf.shape[1] // NC

    def dev(dz, px, pc):
        return {"members": lax.rem(z + dz + nz, nz) * 4 + px * 2 + pc}

    upper = lax.rem(z + 2, nz) < nz // 2
    low = z < nz // 2

    loads = [
        pltpu.make_async_copy(emb_ref.at[pl.ds(j * ch, ch)], stage.at[j], load_sem.at[j]) for j in range(NC)
    ]
    order_in = [j + s for j in range(NC // 2) for s in (0, NC // 2)]
    for j in order_in:
        loads[j].start()
    order_load = pltpu.make_async_copy(order_hbm, order_ref, small_sem.at[0])
    order_load.start()
    thr_load = pltpu.make_async_copy(thr_hbm, thr_ref, small_sem.at[1])
    thr_load.start()

    peers = [dev(0, xo, c), dev(1, x, c), dev(-1, x, c), dev(0, x, co)]
    barrier = pltpu.get_barrier_semaphore()
    for p in peers:
        pl.semaphore_signal(barrier, inc=1, device_id=p, device_id_type=MESH)

    def remote(kind, j, src, dst, target):
        at = kind * NC + j if kind <= DXH else DXH * NC + NC // 2 + kind - DOO
        return pltpu.make_async_remote_copy(
            src_ref=src, dst_ref=dst, send_sem=send_sem.at[kind], recv_sem=recv_sem.at[at],
            device_id=target, device_id_type=MESH,
        )

    def all_of(kind, count):
        some = abuf.at[SO, pl.ds(0, count * ch)]
        return remote(kind, 0, some, some, dev(0, x, co))

    def rows(slot, j):
        return abuf.at[slot, pl.ds(pl.multiple_of(j * ch, ch), ch)]

    def half(base, j, h):
        return bbuf.at[base + lax.div(j, SUB), pl.ds(pl.multiple_of(h * LANES + lax.rem(j, SUB) * ch, ch), ch)]

    def c_m1(j):
        return remote(DM1, j, rows(SO, j), rows(SM1, j), dev(1, x, c))

    def c_p1(j):
        return remote(DP1, j, rows(SO, j), rows(SP1, j), dev(-1, x, c))

    def c_m2(j):
        return remote(DM2, j, rows(SM1, j), rows(SM2, j), dev(1, x, c))

    def c_p2(j):
        return remote(DP2, j, rows(SP1, j), rows(SP2, j), dev(-1, x, c))

    def c_x1(j):
        return remote(DX1, j, rows(SP1, j), half(BX1, j, c), dev(0, xo, c))

    def c_xh_m(i):
        return remote(DXH, i, rows(SM2, i), half(BXH, i, c), dev(0, xo, c))

    def c_xh_p(i):
        return remote(DXH, i, rows(SP2, NC // 2 + i), half(BXH, i, c), dev(0, xo, c))

    def c_oo(j, h):
        return remote(DOO, j, rows(SO, j), half(BO, j, h), dev(0, x, co))

    def c_p1o(j, h):
        return remote(DP1O, j, rows(SP1, j), half(BP1, j, h), dev(0, x, co))

    def c_m1o(j, h):
        return remote(DM1O, j, rows(SM1, j), half(BM1, j, h), dev(0, x, co))

    q_slot = jnp.where(low, SP2, SM2)
    q_off = jnp.where(low, NC // 2, 0)

    def c_qo(i, h):
        return remote(DQO, i, rows(q_slot, q_off + i), half(BQ, i, h), dev(0, x, co))

    def c_fwd(kind, base, j, h):
        return remote(kind, j, half(base, j, h), half(base, j, h), dev(0, x, co))

    def normalise(j):
        loads[j].wait()
        e = stage[j]
        u = (e * lax.rsqrt(jnp.sum(e * e, axis=1, keepdims=True) + 1e-06)).astype(BF16)
        abuf[SO, pl.ds(j * ch, ch)] = u
        bbuf[BO + j // SUB, pl.ds(pl.multiple_of(c * LANES + (j % SUB) * ch, ch), ch)] = u

    normalise(0)
    order_load.wait()
    ordv[c] = order_ref[...]
    pl.semaphore_wait(barrier, len(peers))

    def order_copy(k, src, dst, target):
        return pltpu.make_async_remote_copy(
            src_ref=src, dst_ref=ordv.at[dst], send_sem=vec_sem.at[k], recv_sem=orecv_sem.at[dst],
            device_id=target, device_id_type=MESH,
        )

    def order_wait(slot):
        order_copy(0, order_ref, slot, dev(0, x, co)).wait_recv()

    def order_fwd(slot):
        order_copy(0, ordv.at[slot], slot, dev(0, x, co)).start()

    c_m1(0).start()
    normalise(NC // 2)
    c_p1(NC // 2).start()
    order_copy(0, order_ref, VM1 + c, dev(1, x, c)).start()
    order_copy(0, order_ref, VP1 + c, dev(-1, x, c)).start()
    order_copy(0, order_ref, VO + c, dev(0, x, co)).start()
    for i in range(1, NC // 2):
        normalise(i)
        c_m1(i).start()
        normalise(NC // 2 + i)
        c_p1(NC // 2 + i).start()
    for i in range(NC // 2):
        c_m1(NC // 2 + i).start()
        c_p1(i).start()

    for j in range(NC):
        c_oo(j, c).start()
    racc[...] = jnp.full(racc.shape, -1.0, F32)
    cacc[...] = jnp.full(cacc.shape, -1.0, F32)
    res[...] = jnp.full(res.shape, -1.0, F32)

    order_wait(VM1 + c)
    order_copy(0, ordv.at[VM1 + c], VM2 + c, dev(1, x, c)).start()
    order_fwd(VM1 + c)
    order_wait(VP1 + c)
    order_copy(0, ordv.at[VP1 + c], VP2 + c, dev(-1, x, c)).start()
    order_copy(0, ordv.at[VP1 + c], VX1 + c, dev(0, xo, c)).start()
    order_fwd(VP1 + c)
    order_wait(VX1 + c)
    order_fwd(VX1 + c)
    for base in (VO, VP1, VM1, VX1):
        order_wait(base + co)

    def row_orders(slot, v):
        for j in range(NT):
            line = ordv[v, pl.ds(j, 1)].astype(F32)
            oa[slot, pl.ds(j * LANES, LANES)] = jnp.broadcast_to(line, (LANES, LANES)).T

    def column_orders(base, v, count=NT, off=0):
        for j in range(count):
            for h in (0, 1):
                line = ordv[v + h, pl.ds(j + off, 1)].astype(F32)
                ob[base + j, :, h * LANES : (h + 1) * LANES] = jnp.broadcast_to(line, (8, LANES))

    row_orders(SO, VO + c)
    row_orders(SP1, VP1 + c)
    row_orders(SM1, VM1 + c)
    column_orders(BM1, VM1)
    column_orders(BO, VO)
    column_orders(BP1, VP1)
    column_orders(BX1, VX1)
    xj = jnp.where(upper, 2, 0)

    def tiles(slot, r0, nrows, tile, ntiles, with_columns=True):
        r_sl = pl.ds(r0, nrows) if isinstance(r0, int) else pl.ds(pl.multiple_of(r0, LANES), nrows)
        b = bbuf[pl.ds(tile, ntiles)].reshape(ntiles * 2 * LANES, bbuf.shape[2])
        s = lax.dot_general(abuf[slot, r_sl], b, (((1,), (1,)), ((), ())), preferred_element_type=F32)
        o_rows = oa[slot, r_sl]
        best = racc[slot, r_sl]
        for t in range(ntiles):
            for h in (0, 1):
                k = t * 2 + h
                sk = s[:, k * LANES : (k + 1) * LANES]
                m = ob[tile + t, 0:1, h * LANES : (h + 1) * LANES] < o_rows
                best = jnp.maximum(best, jnp.where(m, sk, -1.0))
                if with_columns:
                    down = jnp.where(m, -1.0, sk).reshape(nrows // 8, 8, LANES)
                    lanes = pl.ds(h * LANES, LANES)
                    cacc[tile + t, :, lanes] = jnp.maximum(cacc[tile + t, :, lanes], jnp.max(down, axis=0))
        racc[slot, r_sl] = best

    nrow = NT * LANES
    two = 2 * LANES

    def whole(slot, tile, with_columns=True):
        tiles(slot, 0, nrow, tile, 1, with_columns)

    def loop(lo, hi, body):
        def step(i, _):
            body(i)
            return 0

        lax.fori_loop(lo, hi, step, 0)

    def turned(t):
        return lax.rem(t + NT // 2, NT)

    def subs(t):
        return [SUB * t + i for i in range(SUB)]

    def first_step(k):
        jp = lax.rem(k + NC // 2, NC)
        c_m1(k).wait_recv()
        c_m2(k).start()
        c_m1o(k, c).start()
        half(BM1, k, c)[...] = rows(SM1, k)[...]
        c_p1(jp).wait_recv()
        c_p2(jp).start()
        c_x1(jp).start()
        c_p1o(jp, c).start()
        half(BP1, jp, c)[...] = rows(SP1, jp)[...]

    def x1_forward(t):
        for j in subs(turned(t)):
            c_x1(j).wait_recv()
            c_fwd(DX1O, BX1, j, c).start()

    def x1_ready(t):
        for j in subs(turned(t)):
            c_fwd(DX1O, BX1, j, co).wait_recv()

    def p1_own(t):
        for j in subs(turned(t)):
            c_p1o(j, co).wait_recv()
        whole(SO, BP1 + turned(t))

    def first(kk):
        for k in subs(kk)[: max(SUB // 2, 1)]:
            first_step(k)

        @pl.when(kk == 0)
        def _():
            all_of(DOO, NC).wait_recv()

        whole(SO, BO + kk, False)

        @pl.when(kk >= 1)
        def _():
            p1_own(kk - 1)

        for k in subs(kk)[max(SUB // 2, 1) :]:
            first_step(k)

        @pl.when(kk >= 1)
        def _():
            x1_forward(kk - 1)

        @pl.when(kk >= 2)
        def _():
            x1_ready(kk - 2)
            whole(SO, BX1 + turned(kk - 2))

    loop(0, NT, first)
    p1_own(NT - 1)
    loop(0, NT, lambda t: whole(SM1, BP1 + t))

    def second_step(k):
        jp = lax.rem(k + NC // 2, NC)
        c_m2(k).wait_recv()
        c_p2(jp).wait_recv()

        @pl.when(k < NC // 2)
        def _():
            c_qo(k, c).start()
            half(BQ, k, c)[...] = rows(q_slot, q_off + k)[...]

        @pl.when(jnp.logical_and(k < NC // 2, upper))
        def _():
            c_xh_p(k).start()

        @pl.when(jnp.logical_and(k < NC // 2, jnp.logical_not(upper)))
        def _():
            c_xh_m(k).start()


    def half_rows(q):
        slot = jnp.where(upper, SM2, SP2)
        tiles(slot, jnp.where(upper, q, 1 - q) * two, two, BXH, 2)

    def q_rows(q):
        tiles(jnp.where(low, SM2, SP2), jnp.where(low, q, 1 - q) * two, two, BQ, 2)

    def row_line(slot, j):
        return jnp.max(racc[slot, pl.ds(j * LANES, LANES)].T, axis=0, keepdims=True)

    def col_line(tile, h):
        return jnp.max(cacc[tile, :, h * LANES : (h + 1) * LANES], axis=0, keepdims=True)

    def result_copy(src, dst, target, k=4):
        return pltpu.make_async_remote_copy(
            src_ref=res.at[src], dst_ref=resin.at[dst], send_sem=vec_sem.at[3], recv_sem=vec_sem.at[k],
            device_id=target, device_id_type=MESH,
        )

    def both_halves(dst, base, slot):
        for j in range(NT):
            line = row_line(slot, j)
            for h in (0, 1):
                res[dst + h, j : j + 1] = jnp.maximum(col_line(base + j, h), jnp.where(c == h, line, -1.0))

    def second(kk):
        for k in subs(kk)[: max(SUB // 2, 1)]:
            second_step(k)

        @pl.when(kk == 0)
        def _():
            order_wait(VM2 + c)
            order_wait(VP2 + c)
            order_fwd(VP2 + c)
            order_fwd(VM2 + c)
            order_copy(0, ordv.at[jnp.where(upper, VP2, VM2) + c], VXH + c, dev(0, xo, c)).start()
            x1_ready(2)
            whole(SO, BX1 + turned(2))

            def one(i):
                whole(SP1 + lax.rem(i, 2), BX1 + turned(lax.div(i, 2)))

            loop(0, 4, one)
            order_wait(VP2 + co)
            order_wait(VM2 + co)
            row_orders(SM2, VM2 + c)
            row_orders(SP2, VP2 + c)
            column_orders(BQ, jnp.where(low, VP2, VM2), 2, jnp.where(low, 2, 0))

        @pl.when(kk == 1)
        def _():
            x1_ready(3)
            loop(SO, SM1 + 1, lambda s: whole(s, BX1 + turned(3)))

        @pl.when(kk == 2)
        def _():
            both_halves(RP1, BP1, SP1)
            for j in range(NT):
                out_ref[0, j : j + 1] = row_line(SO, j)
            order_wait(VXH + c)
            order_fwd(VXH + c)

        @pl.when(kk == 3)
        def _():
            order_wait(VXH + co)
            column_orders(BXH, VXH, 2, xj)
            for h in (0, 1):
                result_copy(RP1 + h, RP1 + c, dev(1, x, h)).start()
            all_of(DXHO, NC // 2).wait_recv()
            half_rows(0)

        for k in subs(kk)[max(SUB // 2, 1) :]:
            second_step(k)

        @pl.when(kk == 0)
        def _():
            x1_forward(3)
            loop(SP1, SM1 + 1, lambda s: whole(s, BX1 + turned(2)))

        @pl.when(jnp.logical_or(kk == 1, kk == 2))
        def _():
            for i in subs(kk - 1):
                c_xh_m(i).wait_recv()
                c_fwd(DXHO, BXH, i, c).start()

        @pl.when(kk == 1)
        def _():
            all_of(DM1O, NC).wait_recv()
            all_of(DQO, NC // 2).wait_recv()
            tiles(SM2, 0, two, BX1, NT)
            tiles(SP2, two, two, BM1, NT)
            q_rows(0)

    loop(0, NT, second)

    tiles(SM2, two, two, BX1, NT)
    for h in (0, 1):
        for j in range(NT):
            res[RX1 + h, j : j + 1] = col_line(BX1 + j, h)
    half_rows(1)
    for h in (0, 1):
        result_copy(RX1 + h, RX1 + c, dev(1, xo, h)).start()
        for i in (0, 1):
            res[RXHM + h, pl.ds(xj + i, 1)] = col_line(BXH + i, h)
    tiles(SP2, 0, two, BM1, NT)

    @pl.when(upper)
    def _():
        for h in (0, 1):
            result_copy(RXHM + h, RXHP + c, dev(2, xo, h), 5).start()

    @pl.when(jnp.logical_not(upper))
    def _():
        for h in (0, 1):
            result_copy(RXHM + h, RXHM + c, dev(-2, xo, h), 5).start()

    both_halves(RM1, BM1, SM1)
    q_rows(1)
    for h in (0, 1):
        result_copy(RM1 + h, RM1 + c, dev(-1, x, h)).start()

    for j in range(NT):
        for dst, slot in ((RM2, SM2), (RP2, SP2)):
            res[dst + c, j : j + 1] = row_line(slot, j)
    for h in (0, 1):
        for i in (0, 1):
            at, line = jnp.where(low, RP2, RM2) + h, pl.ds(jnp.where(low, 2, 0) + i, 1)
            res[at, line] = jnp.maximum(res[at, line], col_line(BQ + i, h))
    for h in (0, 1):
        result_copy(RM2 + h, RM2 + c, dev(-2, x, h)).start()
        result_copy(RP2 + h, RP2 + c, dev(2, x, h)).start()

    for kind in range(ND):
        all_of(kind, NC // 2 if kind in (DXH, DXHO, DQO) else NC).wait_send()
    some = ordv.at[pl.ds(0, 13)]
    pltpu.make_async_remote_copy(
        src_ref=some, dst_ref=some, send_sem=vec_sem.at[0], recv_sem=orecv_sem.at[0],
        device_id=dev(0, x, co), device_id_type=MESH,
    ).wait_send()
    result_copy(pl.ds(0, RXHM), pl.ds(0, RXHM), dev(1, x, c)).wait_recv()
    thr_load.wait()
    best = out_ref[0]
    for slot in range(RXHM):
        best = jnp.maximum(best, resin[slot])
    out_ref[0] = best
    out_ref[1] = jnp.maximum(best - thr_ref[...], 0.0)

    @pl.when(low)
    def _():
        result_copy(pl.ds(0, NR - RXHM), pl.ds(RXHM, NR - RXHM), dev(1, x, c), 5).wait_recv()
        more = out_ref[0]
        for slot in range(RXHM, NR):
            more = jnp.maximum(more, resin[slot])
        out_ref[0] = more
        out_ref[1] = jnp.maximum(more - thr_ref[...], 0.0)

    result_copy(pl.ds(0, NSRC), pl.ds(0, NSRC), dev(1, x, c)).wait_send()


def shards(embeddings, member_order, threshold):
    r, e = embeddings.shape
    out = pl.pallas_call(
        kernel,
        out_shape=jax.ShapeDtypeStruct((2, NT, LANES), F32),
        in_specs=[pl.BlockSpec(memory_space=pl.ANY)] * 3,
        out_specs=pl.BlockSpec(memory_space=pltpu.VMEM),
        scratch_shapes=[
            pltpu.VMEM((NT, LANES), jnp.int32),
            pltpu.VMEM((1, 1), F32),
            pltpu.VMEM((NC, r // NC, e), F32),
            pltpu.VMEM((NS, r, e), BF16),
            pltpu.VMEM((NB, 2 * LANES, e), BF16),
            pltpu.VMEM((NS, r, LANES), F32),
            pltpu.VMEM((NB, 8, 2 * LANES), F32),
            pltpu.VMEM((NS, r, LANES), F32),
            pltpu.VMEM((NB, 8, 2 * LANES), F32),
            pltpu.VMEM((NV, NT, LANES), jnp.int32),
            pltpu.VMEM((NSRC, NT, LANES), F32),
            pltpu.VMEM((NR, NT, LANES), F32),
            pltpu.SemaphoreType.DMA((NC,)),
            pltpu.SemaphoreType.DMA((2,)),
            pltpu.SemaphoreType.DMA((ND,)),
            pltpu.SemaphoreType.DMA((DXH * NC + NC // 2 + ND - DOO,)),
            pltpu.SemaphoreType.DMA((6,)),
            pltpu.SemaphoreType.DMA((NV,)),
        ],
        compiler_params=pltpu.CompilerParams(
            collective_id=0, has_side_effects=True, vmem_limit_bytes=52 * 1024 * 1024
        ),
    )(member_order.reshape(NT, LANES), threshold.reshape(1, 1), embeddings)
    return out[0].reshape(r), out[1].reshape(r)


def solution(mesh):
    placed = (P(("clusters", "members"), None), P(("clusters", "members")), P("clusters"))
    return jax.shard_map(
        shards,
        mesh=mesh,
        in_specs=placed,
        out_specs=(P(("clusters", "members")), P(("clusters", "members"))),
        check_vma=False,
    )
```
